256 devices in a mesh: cluster: 8 (over x, core), leaf: 32 (over y, z).
Axes of the slice: x: 4, y: 4, z: 8, core: 2. Of those that a mesh axis runs over, the one named last changes fastest.
Arguments:
- probes: float32 [262144, 512], P(('cluster', 'leaf')), may hold values from -6 to 6
- dense_leaf: float32 [262144, 1024], P(('cluster', 'leaf')), may hold values from -0.1875 to 0.1875
- leaf_basis: float32 [262144, 128], P(('cluster', 'leaf')), may hold values from -0.1875 to 0.1875
- sibling_cores: float32 [256, 32, 128, 128], P(('cluster', 'leaf')), may hold values from -0.25 to 0.25
- transfer: float32 [256, 128, 128], P(('cluster', 'leaf')), may hold values from -0.5 to 0.5
- cluster_cores: float32 [8, 8, 128, 128], P('cluster'), may hold values from -0.0625 to 0.0625
Outputs:
- product: float32 [262144, 512], P(('cluster', 'leaf'))
The draws below stay inside these ranges and needn't reach their ends.
All inputs are finite; a program needn't handle non-finite values.
Results may differ from the reference program's by a relative error of at most 0.00005.
Values sent between devices are 32-bit elements; how exact they have to be, the bound alone decides.
A program may use at most 128 MiB of HBM per device.

```python
import jax
import jax.numpy as jnp
from jax import lax

LEAF = 1024
R = 128
R2 = 128
P_SIZE = 512
LEAVES = 256
ORDER = 262144
N_CLUSTER = 8
N_LEAF = 32


def levels(own_key, shape, cuts, least, largest):
    level = 1.0
    for position, blocks in cuts:
        steps = jax.random.uniform(jax.random.fold_in(jax.random.fold_in(own_key, 6), position), (blocks,), jnp.float32, least / len(cuts), largest / len(cuts))
        level = level * jnp.repeat(jnp.exp(steps), shape[position] // blocks).reshape((-1,) + (1,) * (len(shape) - 1 - position))
    return level


def scatter_about(key, extent, deviation, most, split=(), held_as=jnp.bfloat16):
    entries = jax.random.normal(key, extent, jnp.float32) * deviation
    if len(split) > 0:
        entries = levels(key, extent, split, -0.22, 0.18) * entries
    return jnp.clip(entries, min=-most, max=most).astype(held_as)


def setup_inputs(seed: int = 0) -> dict:
    arg_keys = jax.random.split(jax.random.key(seed), 7)
    return {
        "probes": scatter_about(arg_keys[0], (ORDER, P_SIZE), 1.0, 6.0, ((0, 256),), jnp.float32),
        "dense_leaf": scatter_about(arg_keys[1], (ORDER, LEAF), LEAF ** -0.5, 0.1875, ((0, 256),), jnp.float32),
        "leaf_basis": scatter_about(arg_keys[2], (ORDER, R), LEAF ** -0.5, 0.1875, ((0, 256),), jnp.float32),
        "sibling_cores": scatter_about(arg_keys[3], (LEAVES, N_LEAF, R, R), (R * N_LEAF // 8) ** -0.5, 0.25, ((0, 256),), jnp.float32),
        "transfer": scatter_about(arg_keys[4], (LEAVES, R, R2), R ** -0.5, 0.5, ((0, 256),), jnp.float32),
        "cluster_cores": scatter_about(arg_keys[5], (N_CLUSTER, N_CLUSTER, R2, R2), (R2 * N_CLUSTER * N_LEAF // 4) ** -0.5, 0.0625, ((0, 8),), jnp.float32),
    }


HI = lax.Precision.HIGHEST


def reference(probes, dense_leaf, leaf_basis, sibling_cores, transfer, cluster_cores):
    nclu = N_CLUSTER
    nleaf = N_LEAF
    xl = probes.reshape(nclu, nleaf, LEAF, P_SIZE)
    dl = dense_leaf.reshape(nclu, nleaf, LEAF, LEAF)
    ul = leaf_basis.reshape(nclu, nleaf, LEAF, R)
    near = jnp.einsum('cnab,cnbp->cnap', dl, xl, precision=HI) + jnp.einsum('cnba,cnbp->cnap', dl, xl, precision=HI)
    coef = jnp.einsum('cnar,cnap->cnrp', ul, xl, precision=HI)
    keep = (1.0 - jnp.eye(nleaf, dtype=jnp.float32))[None, :, :, None, None]
    cores = sibling_cores.reshape(nclu, nleaf, nleaf, R, R) * keep
    sib = jnp.einsum('cijab,cjbp->ciap', cores, coef, precision=HI) + jnp.einsum('cjiba,cjbp->ciap', cores, coef, precision=HI)
    el = transfer.reshape(nclu, nleaf, R, R2)
    g = jnp.sum(jnp.einsum('cnrs,cnrp->cnsp', el, coef, precision=HI), axis=1)
    bkeep = (1.0 - jnp.eye(nclu, dtype=jnp.float32))[:, :, None, None]
    bm = cluster_cores * bkeep
    h = jnp.einsum('cdab,dbp->cap', bm, g, precision=HI) + jnp.einsum('dcba,dbp->cap', bm, g, precision=HI)
    total = sib + jnp.einsum('cnrs,csp->cnrp', el, h, precision=HI)
    out = near + jnp.einsum('cnar,cnrp->cnap', ul, total, precision=HI)
    return out.reshape(nclu * nleaf * LEAF, P_SIZE)
```

```python
import jax
import jax.numpy as jnp
from jax import lax
from jax.experimental import pallas as pl
from jax.experimental.pallas import tpu as pltpu
from jax.sharding import PartitionSpec as P

MESH = pl.DeviceIdType.MESH
F32, BF16 = jnp.float32, jnp.bfloat16
NY, NZ, NC = 4, 8, 8
LEAF, R, PC = 1024, 128, 512
HALF = PC // 2
NN = (((1,), (0,)), ((), ()))
NT = (((1,), (1,)), ((), ()))


def split(v):
    hi = v.astype(BF16)
    return hi, (v - hi.astype(F32)).astype(BF16)


def dot3(a, b, dims):
    (ah, al), (bh, bl) = a, b

    def one(u, v):
        return lax.dot_general(u, v, dims, preferred_element_type=F32)

    return one(ah, bh) + one(ah, bl) + one(al, bh)


GROUPS = ((4,), (3, 5), (2, 6), (1, 7), (0,))
LENGTH = {(1, 0): 4, (1, 1): 3, (-1, 0): 3, (-1, 1): 4}
CHAINS = tuple(LENGTH)


def kernel(
    x_hbm, d_hbm, u_hbm, a_hbm, e_hbm, b_hbm, out_hbm,
    xv, dv, uv, xh, xl, a2, ah, al, cc, cr, crh, crl, er, bv, p2, rz, p1, ry, near, gs, gz, gp, gx, ts, tx, hp, hz, hy, tot,
    lsem, ssem, rsem,
):
    leaf = lax.axis_index("leaf")
    clu = lax.axis_index("cluster")
    y, z = leaf // NZ, lax.rem(leaf, NZ)
    counts = {"local": 0, "remote": 0}
    started = []

    def at_y(d):
        return {"leaf": lax.rem(y + d + NY, NY) * NZ + z}

    def at_z(d):
        return {"leaf": y * NZ + lax.rem(z + d + NZ, NZ)}

    def at_c(d):
        return {"cluster": lax.rem(clu + d + NC, NC)}

    barrier = pltpu.get_barrier_semaphore()
    partners = [at_y(d) for d in range(1, NY)] + [at_z(d) for d in range(1, NZ)] + [at_c(d) for d in range(1, NC)]
    for partner in partners:
        pl.semaphore_signal(barrier, inc=1, device_id=partner, device_id_type=MESH)

    def load(src, dst):
        i = counts["local"]
        counts["local"] += 1
        copy = pltpu.make_async_copy(src, dst, lsem.at[i])
        copy.start()
        return copy

    def send(src, dst, where):
        i = counts["remote"]
        counts["remote"] += 1
        copy = pltpu.make_async_remote_copy(
            src_ref=src, dst_ref=dst, send_sem=ssem.at[i], recv_sem=rsem.at[i], device_id=where, device_id_type=MESH
        )
        copy.start()
        started.append(copy)
        return copy

    load_x = load(x_hbm, xv)
    load_u = load(u_hbm, uv)
    load_d = load(d_hbm, dv)
    load_e = load(e_hbm.at[0], er.at[0])
    own_a = {d: load(a_hbm.at[0, y * NZ + lax.rem(z + d, NZ)], a2.at[0, d]) for d in range(1, NZ)}
    load_b = [load(b_hbm.at[0, lax.rem(clu - d + NC, NC)], bv.at[d]) for d in range(1, NC)]
    a2[0, 0] = jnp.zeros((R, R), F32)

    load_x.wait()
    load_u.wait()
    h, l = split(xv[...])
    xh[...] = h
    xl[...] = l
    coef = dot3(split(uv[...].T), (xh[...], xl[...]), NN).T
    cc[0] = coef
    cr[0] = coef

    pl.semaphore_wait(barrier, len(partners))

    def rows(half):
        return pl.ds(half * HALF, HALF)

    def slot(sign, step):
        return step if sign < 0 else (NZ - step) % NZ

    gather = {}

    def gather_step(chain, step):
        sign, half = chain
        gather[chain, step] = send(
            cc.at[slot(sign, step - 1), rows(half)], cc.at[slot(sign, step), rows(half)], at_z(sign)
        )

    for chain in CHAINS:
        gather_step(chain, 1)

    cores = {}

    def send_cores(d):
        for dy in (1, 3, 2):
            target = lax.rem(y + dy, NY) * NZ + lax.rem(z + d, NZ)
            cores[d, dy] = send(a_hbm.at[0, target], a2.at[NY - dy, d], at_y(dy))

    send_cores(4)
    rows_y = [send(cc.at[0], cr.at[NY - dy], at_y(dy)) for dy in (1, 3, 2)]
    maps_y = [send(e_hbm.at[0], er.at[NY - dy], at_y(dy)) for dy in (1, 3, 2)]
    for group in GROUPS[1:]:
        for d in group:
            send_cores(d)

    def relay(step):
        for chain in CHAINS:
            if step < LENGTH[chain]:
                gather[chain, step].wait_recv()
                gather_step(chain, step + 1)

    def near_chunk(i):
        size = LEAF // 4
        part = slice(i * size, (i + 1) * size)
        sym = dv[part, :] + dv[:, part].T
        near[part, :] = dot3(split(sym), (xh[...], xl[...]), NN)

    load_d.wait()
    near_chunk(0)
    relay(1)
    near_chunk(1)
    relay(2)
    near_chunk(2)

    for copy in rows_y + maps_y:
        copy.wait_recv()
    load_e.wait()
    mine = pl.ds(pl.multiple_of(y * R, R), R)
    g = jnp.zeros((R, R), F32)
    for r in range(NY):
        h, l = split(cr[r])
        crh[:, r * R : (r + 1) * R] = h
        crl[:, r * R : (r + 1) * R] = l
        g = g + dot3(split(cr[r, mine, :]), split(er[r]), NN)
    gs[...] = g
    PIECE = R // NZ

    def piece(at):
        return pl.ds(pl.multiple_of(at * PIECE, PIECE), PIECE)

    g_z = [send(gs.at[piece(lax.rem(z + d, NZ))], gz.at[d], at_z(d)) for d in range(1, NZ)]

    sums = {}

    def second(group):
        for d in group:
            for dy in (1, 3, 2):
                cores[d, dy].wait_recv()
            if d > 0:
                own_a[d].wait()
        for i, d in enumerate(group):
            h, l = split(a2[:, d].reshape(NY * R, R))
            ah[d] = h
            al[d] = l
        b = tuple(jnp.concatenate([m[d] for d in group], axis=1) for m in (ah, al))
        t = dot3((crh[...], crl[...]), b, NN)
        for i, d in enumerate(group):
            p2[d] = t[:, i * R : (i + 1) * R]

    def sum_step(chain, step):
        sign, half = chain
        left = LENGTH[chain] - step
        at = (sign * left) % NZ
        index = CHAINS.index(chain)
        if step > 0:
            sums[chain, step].wait_recv()
            p2[at, rows(half)] = p2[at, rows(half)] + rz[index, step - 1]
        sums[chain, step + 1] = send(p2.at[at, rows(half)], rz.at[index, step], at_z(sign))

    second(GROUPS[0])
    for chain in CHAINS:
        if LENGTH[chain] == 4:
            sum_step(chain, 0)
    second(GROUPS[1])
    for chain in CHAINS:
        if LENGTH[chain] == 3:
            sum_step(chain, 0)
    relay(3)

    for copy in g_z:
        copy.wait_recv()
    own_piece = gs[piece(z), :]
    for d in range(1, NZ):
        own_piece = own_piece + gz[d]
    gp[...] = own_piece
    g_c = [send(gp, gx.at[d], at_c(d)) for d in range(1, NC)]
    for copy in load_b:
        copy.wait()
    halves = split(own_piece)
    for d in range(1, NC):
        ts[d] = dot3(halves, split(bv[d]), NN)
    t_c = [send(ts.at[d], tx.at[d], at_c(-d)) for d in range(1, NC)]

    near_chunk(3)
    second(GROUPS[2])
    for chain in CHAINS:
        sum_step(chain, 1)

    for copy in g_c + t_c:
        copy.wait_recv()
    field = tx[1]
    for d in range(2, NC):
        field = field + tx[d]
    for d in range(1, NC):
        field = field + dot3(split(gx[d]), split(bv[d]), NT)
    hp[...] = field
    hz[piece(z), :] = field
    h_z = [send(hp, hz.at[piece(z)], at_z(d)) for d in range(1, NZ)]

    second(GROUPS[3])
    for chain in CHAINS:
        sum_step(chain, 2)

    for chain in CHAINS:
        gather[chain, LENGTH[chain]].wait_recv()

    def first(group, fresh):
        a = split(jnp.concatenate([cc[d] for d in group], axis=1))
        b = tuple(jnp.concatenate([m[d] for d in group], axis=1) for m in (ah, al))
        t = dot3(a, b, NT)
        for r in range(NY):
            new = t[:, r * R : (r + 1) * R]
            p1[r] = new if fresh else p1[r] + new

    first(GROUPS[0], True)
    first(GROUPS[1], False)

    for copy in h_z:
        copy.wait_recv()
    hy[mine, :] = hz[...]
    h_y = [send(hz, hy.at[mine], at_y(dy)) for dy in (1, 3, 2)]
    first(GROUPS[2], False)

    for chain in CHAINS:
        if LENGTH[chain] == 4:
            sum_step(chain, 3)
    first(GROUPS[3], False)
    second(GROUPS[4])
    first(GROUPS[4], False)
    sums_y = [send(p1.at[dy], ry.at[dy], at_y(dy)) for dy in (1, 3, 2)]

    total = p1[0] + p2[0]
    for copy in h_y:
        copy.wait_recv()
    total = total + dot3(split(hy[...]), split(er[0]), NT)
    tot[...] = total
    for chain in CHAINS:
        length = LENGTH[chain]
        sums[chain, length].wait_recv()
        half = rows(chain[1])
        tot[half, :] = tot[half, :] + rz[CHAINS.index(chain), length - 1]
    for copy in sums_y:
        copy.wait_recv()
    total = split(tot[...] + ry[1] + ry[2] + ry[3])
    writes = []
    for i in range(4):
        part = slice(i * 256, (i + 1) * 256)
        near[part, :] = near[part, :] + dot3(split(uv[part, :]), total, NT)
        writes.append(load(near.at[part], out_hbm.at[part]))
    for copy in started:
        copy.wait_send()
    for copy in writes:
        copy.wait()


N_LOCAL, N_REMOTE = 32, 112


def local(probes, dense_leaf, leaf_basis, sibling_cores, transfer, cluster_cores):
    hbm = pl.BlockSpec(memory_space=pl.ANY)
    vmem = pltpu.VMEM
    scratch = [
        vmem((LEAF, PC), F32), vmem((LEAF, LEAF), F32), vmem((LEAF, R), F32), vmem((LEAF, PC), BF16), vmem((LEAF, PC), BF16),
        vmem((NY, NZ, R, R), F32), vmem((NZ, NY * R, R), BF16), vmem((NZ, NY * R, R), BF16),
        vmem((NZ, PC, R), F32), vmem((NY, PC, R), F32), vmem((PC, NY * R), BF16), vmem((PC, NY * R), BF16),
        vmem((NY, R, R), F32), vmem((NC, R, R), F32),
        vmem((NZ, PC, R), F32), vmem((4, 4, HALF, R), F32), vmem((NY, PC, R), F32), vmem((NY, PC, R), F32), vmem((LEAF, PC), F32),
        vmem((R, R), F32), vmem((NZ, R // NZ, R), F32), vmem((R // NZ, R), F32), vmem((NC, R // NZ, R), F32),
        vmem((NC, R // NZ, R), F32), vmem((NC, R // NZ, R), F32), vmem((R // NZ, R), F32), vmem((R, R), F32), vmem((PC, R), F32),
        vmem((PC, R), F32),
        pltpu.SemaphoreType.DMA((N_LOCAL,)), pltpu.SemaphoreType.DMA((N_REMOTE,)), pltpu.SemaphoreType.DMA((N_REMOTE,)),
    ]
    return pl.pallas_call(
        kernel,
        out_shape=jax.ShapeDtypeStruct((LEAF, PC), F32),
        in_specs=[hbm] * 6,
        out_specs=hbm,
        scratch_shapes=scratch,
        compiler_params=pltpu.CompilerParams(collective_id=0, has_side_effects=True, vmem_limit_bytes=60 * 2**20),
    )(probes, dense_leaf, leaf_basis, sibling_cores, transfer, cluster_cores)


def solution(mesh):
    both = P(("cluster", "leaf"), None)
    return jax.shard_map(
        local,
        mesh=mesh,
        in_specs=(
            both, both, both, P(("cluster", "leaf"), None, None, None), P(("cluster", "leaf"), None, None),
            P("cluster", None, None, None),
        ),
        out_specs=both,
        check_vma=False,
    )
```

```python
import jax
import jax.numpy as jnp
from jax import lax
from jax.experimental import pallas as pl
from jax.experimental.pallas import tpu as pltpu
from jax.sharding import PartitionSpec as P

MESH = pl.DeviceIdType.MESH
F32, BF16 = jnp.float32, jnp.bfloat16
NY, NZ, NC = 4, 8, 8
LEAF, R, PC = 1024, 128, 512
HALF = PC // 2
NN = (((1,), (0,)), ((), ()))
NT = (((1,), (1,)), ((), ()))


def split(v):
    hi = v.astype(BF16)
    return hi, (v - hi.astype(F32)).astype(BF16)


def dot3(a, b, dims):
    (ah, al), (bh, bl) = a, b

    def one(u, v):
        return lax.dot_general(u, v, dims, preferred_element_type=F32)

    return one(ah, bh) + one(ah, bl) + one(al, bh)


GROUPS = ((4,), (3, 5), (2, 6), (1, 7))
QUARTERS, QROWS = 4, PC // 4
PIECE = R // NZ
ORDER = {1: (0, 1, 2, 3), -1: (2, 3, 0, 1)}


def steps(sign, quarter, size):
    return size // 2 if quarter in ORDER[sign][:2] else size // 2 - 1


def kernel(
    x_hbm, d_hbm, u_hbm, a_hbm, e_hbm, b_hbm, near_out, tot_out,
    near, tot, av, xv, dv, uv, xh, xl, a2, ah, al, cc, cr, crh, crl, er, bv, p2, rz, p1, ry, gs, gz, gp, gx, ts, tx, hp, hz, hy,
    lsem, ssem, rsem,
):
    leaf = lax.axis_index("leaf")
    clu = lax.axis_index("cluster")
    y, z = leaf // NZ, lax.rem(leaf, NZ)
    counts = {"local": 0, "remote": 0}
    started = []

    def at_y(d):
        return {"leaf": lax.rem(y + d + NY, NY) * NZ + z}

    def at_z(d):
        return {"leaf": y * NZ + lax.rem(z + d + NZ, NZ)}

    def at_c(d):
        return {"cluster": lax.rem(clu + d + NC, NC)}

    barrier = pltpu.get_barrier_semaphore()
    partners = [at_y(d) for d in range(1, NY)] + [at_z(d) for d in range(1, NZ)] + [at_c(d) for d in range(1, NC)]
    for partner in partners:
        pl.semaphore_signal(barrier, inc=1, device_id=partner, device_id_type=MESH)

    def load(src, dst):
        i = counts["local"]
        counts["local"] += 1
        copy = pltpu.make_async_copy(src, dst, lsem.at[i])
        copy.start()
        return copy

    def send(src, dst, where):
        i = counts["remote"]
        counts["remote"] += 1
        copy = pltpu.make_async_remote_copy(
            src_ref=src, dst_ref=dst, send_sem=ssem.at[i], recv_sem=rsem.at[i], device_id=where, device_id_type=MESH
        )
        copy.start()
        started.append(copy)
        return copy

    load_x = load(x_hbm, xv)
    load_u = load(u_hbm, uv)
    load_d = load(d_hbm, dv)
    load_e = load(e_hbm.at[0], er.at[0])
    load_a = load(a_hbm.at[0], av)
    own_a = {d: load(a_hbm.at[0, y * NZ + lax.rem(z + d, NZ)], a2.at[0, d]) for d in range(1, NZ)}
    own_y = [load(a_hbm.at[0, lax.rem(y + d, NY) * NZ + z], a2.at[d, 0]) for d in range(1, NY)]
    load_b = [load(b_hbm.at[0, lax.rem(clu - d + NC, NC)], bv.at[d]) for d in range(1, NC)]

    load_x.wait()
    load_u.wait()
    h, l = split(xv[...])
    xh[...] = h
    xl[...] = l
    coef = dot3(split(uv[...].T), (xh[...], xl[...]), NN).T
    cc[0] = coef
    cr[0] = coef

    pl.semaphore_wait(barrier, len(partners))

    def rows(quarter):
        return pl.ds(quarter * QROWS, QROWS)

    moves = {}

    def gather_step(ref, size, where, sign, quarter, step):
        def slot(n):
            return (-sign * n) % size

        moves[size, sign, quarter, step] = send(
            ref.at[slot(step - 1), rows(quarter)], ref.at[slot(step), rows(quarter)], where(sign)
        )

    def gather_event(ref, size, where, k):
        step, place = k // QUARTERS + 1, k % QUARTERS
        for sign in (1, -1):
            quarter = ORDER[sign][place]
            if step <= steps(sign, quarter, size):
                moves[size, sign, quarter, step].wait_recv()
                if step < steps(sign, quarter, size):
                    gather_step(ref, size, where, sign, quarter, step + 1)

    def z_event(k):
        gather_event(cc, NZ, at_z, k)

    def y_event(k):
        gather_event(cr, NY, at_y, k)

    for place in range(QUARTERS):
        for sign in (1, -1):
            gather_step(cc, NZ, at_z, sign, ORDER[sign][place], 1)
        for sign in (1, -1):
            gather_step(cr, NY, at_y, sign, ORDER[sign][place], 1)

    cores = {}

    def send_cores(group):
        for d in group:
            for dy in (2, 1, 3):
                target = lax.rem(y + dy, NY) * NZ + lax.rem(z + d, NZ)
                cores[d, dy] = send(av.at[target], a2.at[NY - dy, d], at_y(dy))

    writes = []

    def near_chunk(i):
        size = LEAF // 4
        part = slice(i * size, (i + 1) * size)
        sym = dv[part, :] + dv[:, part].T
        near[part, :] = dot3(split(sym), (xh[...], xl[...]), NN)
        writes.append(load(near.at[part], near_out.at[part]))

    def send_maps():
        return [send(er.at[0], er.at[NY - dy], at_y(dy)) for dy in (1, 3, 2)]

    load_e.wait()
    maps_y = send_maps()
    load_d.wait()
    near_chunk(0)
    near_chunk(1)
    z_event(0)
    y_event(0)
    z_event(1)
    y_event(1)
    load_a.wait()
    send_cores(GROUPS[0])
    z_event(2)
    near_chunk(2)
    z_event(3)
    near_chunk(3)
    z_event(4)
    for copy in own_y:
        copy.wait()
    own_h, own_l = split(jnp.concatenate([a2[d, 0] for d in range(1, NY)], axis=1))
    h, l = split(cr[0])
    crh[:, :R] = h
    crl[:, :R] = l
    t = dot3((crh[:, :R], crl[:, :R]), (own_h, own_l), NN)
    for d in range(1, NY):
        p1[d] = t[:, (d - 1) * R : d * R]
    z_event(5)
    y_event(2)
    y_event(3)
    send_cores(GROUPS[1])
    z_event(6)
    y_event(4)
    y_event(5)
    send_cores(GROUPS[2])
    send_cores(GROUPS[3])

    for r in range(1, NY):
        h, l = split(cr[r])
        crh[:, r * R : (r + 1) * R] = h
        crl[:, r * R : (r + 1) * R] = l
    z_event(7)

    for copy in maps_y:
        copy.wait_recv()
    mine = pl.ds(pl.multiple_of(y * R, R), R)
    g = jnp.zeros((R, R), F32)
    for r in range(NY):
        g = g + dot3(split(cr[r, mine, :]), split(er[r]), NN)
    gs[...] = g

    def piece(at):
        return pl.ds(pl.multiple_of(at * PIECE, PIECE), PIECE)

    g_z = [send(gs.at[piece(lax.rem(z + d, NZ))], gz.at[d], at_z(d)) for d in (4, 3, 5, 2, 6, 1, 7)]
    z_event(8)
    p2[0] = dot3((crh[:, R:], crl[:, R:]), (own_h, own_l), NT)
    z_event(9)

    def second(group):
        for d in group:
            for dy in (2, 1, 3):
                cores[d, dy].wait_recv()
            own_a[d].wait()
            h, l = split(a2[:, d].reshape(NY * R, R))
            ah[d] = h
            al[d] = l
        b = tuple(jnp.concatenate([m[d] for d in group], axis=1) for m in (ah, al))
        t = dot3((crh[...], crl[...]), b, NN)
        for i, d in enumerate(group):
            p2[d] = t[:, i * R : (i + 1) * R]

    sums = {}

    def sum_step(sign, quarter, step):
        length = steps(sign, quarter, NZ)
        at = (sign * (length - step)) % NZ
        way = 0 if sign > 0 else 1
        if step > 0:
            sums[sign, quarter, step].wait_recv()
            p2[at, rows(quarter)] = p2[at, rows(quarter)] + rz[way, quarter, step - 1]
        sums[sign, quarter, step + 1] = send(p2.at[at, rows(quarter)], rz.at[way, quarter, step], at_z(sign))

    def sum_steps(places, step):
        for place in places:
            for sign in (1, -1):
                sum_step(sign, ORDER[sign][place], step)

    def first(group, fresh, part=range(NY)):
        a = split(jnp.concatenate([cc[d] for d in group], axis=1))
        b = tuple(jnp.concatenate([m[d, part[0] * R : (part[-1] + 1) * R] for d in group], axis=1) for m in (ah, al))
        t = dot3(a, b, NT)
        for i, r in enumerate(part):
            new = t[:, i * R : (i + 1) * R]
            p1[r] = new if fresh and r == 0 else p1[r] + new

    second(GROUPS[0])
    sum_steps((0, 1), 0)

    for copy in g_z:
        copy.wait_recv()
    own_piece = gs[piece(z), :]
    for d in range(1, NZ):
        own_piece = own_piece + gz[d]
    gp[...] = own_piece
    g_c = [send(gp, gx.at[d], at_c(d)) for d in range(1, NC)]
    for copy in load_b:
        copy.wait()
    halves = split(own_piece)
    for d in range(1, NC):
        ts[d] = dot3(halves, split(bv[d]), NN)
    t_c = [send(ts.at[d], tx.at[d], at_c(-d)) for d in range(1, NC)]

    second(GROUPS[1])
    sum_steps((2, 3), 0)
    sum_steps((0, 1), 1)

    for copy in g_c + t_c:
        copy.wait_recv()
    field = tx[1]
    for d in range(2, NC):
        field = field + tx[d]
    for d in range(1, NC):
        field = field + dot3(split(gx[d]), split(bv[d]), NT)
    hp[...] = field
    hz[piece(z), :] = field
    h_z = [send(hp, hz.at[piece(z)], at_z(d)) for d in (4, 3, 5, 2, 6, 1, 7)]

    for k in range(10, 14):
        z_event(k)
    first(GROUPS[0], True)

    second(GROUPS[2])
    sum_steps((2, 3), 1)
    sum_steps((0, 1), 2)
    first(GROUPS[1], False)
    first(GROUPS[2], False)

    for copy in h_z:
        copy.wait_recv()
    hy[mine, :] = hz[...]
    h_y = [send(hz, hy.at[mine], at_y(dy)) for dy in (1, 3, 2)]
    second(GROUPS[3])

    sums_y = {}

    def sum_y(sign, quarter, step):
        length = steps(sign, quarter, NY)
        at = (sign * (length - step)) % NY
        way = 0 if sign > 0 else 1
        if step > 0:
            sums_y[sign, quarter, step].wait_recv()
            p1[at, rows(quarter)] = p1[at, rows(quarter)] + ry[way, quarter, step - 1]
        sums_y[sign, quarter, step + 1] = send(p1.at[at, rows(quarter)], ry.at[way, quarter, step], at_y(sign))

    first(GROUPS[3], False, range(2, 4))
    for place in (0, 1):
        for sign in (1, -1):
            sum_y(sign, ORDER[sign][place], 0)
    first(GROUPS[3], False, range(0, 2))
    for place in (2, 3):
        for sign in (1, -1):
            sum_y(sign, ORDER[sign][place], 0)
    sum_steps((2, 3), 2)
    sum_steps((0, 1), 3)
    for place in (0, 1):
        for sign in (1, -1):
            sum_y(sign, ORDER[sign][place], 1)

    for copy in h_y:
        copy.wait_recv()
    total = p1[0] + p2[0] + dot3(split(hy[...]), split(er[0]), NT)
    tot[...] = total
    for place in (2, 3, 0, 1):
        for sign in (1, -1):
            quarter = ORDER[sign][place]
            length = steps(sign, quarter, NZ)
            sums[sign, quarter, length].wait_recv()
            tot[rows(quarter), :] = tot[rows(quarter), :] + rz[0 if sign > 0 else 1, quarter, length - 1]
    for place in (2, 3, 0, 1):
        for sign in (1, -1):
            quarter = ORDER[sign][place]
            length = steps(sign, quarter, NY)
            sums_y[sign, quarter, length].wait_recv()
            tot[rows(quarter), :] = tot[rows(quarter), :] + ry[0 if sign > 0 else 1, quarter, length - 1]
    writes.append(load(tot, tot_out))
    for copy in started:
        copy.wait_send()
    for copy in writes:
        copy.wait()


def last(near, u, tot, out, held, sems):
    total = split(tot[...])
    copies = []
    for i in range(4):
        part = pl.ds(i * (LEAF // 4), LEAF // 4)
        held[part, :] = near[part, :] + dot3(split(u[part, :]), total, NT)
        copies.append(pltpu.make_async_copy(held.at[part], out.at[part], sems.at[i]))
        copies[-1].start()
    for copy in copies:
        copy.wait()


N_LOCAL, N_REMOTE = 32, 144


def local(probes, dense_leaf, leaf_basis, sibling_cores, transfer, cluster_cores):
    arrays = (probes, dense_leaf, leaf_basis, sibling_cores, transfer, cluster_cores)
    hbm = pl.BlockSpec(memory_space=pltpu.HBM)
    vmem = pltpu.VMEM
    scratch = [
        vmem((LEAF, PC), F32), vmem((PC, R), F32), vmem((NY * NZ, R, R), F32), vmem((LEAF, PC), F32), vmem((LEAF, LEAF), F32), vmem((LEAF, R), F32), vmem((LEAF, PC), BF16), vmem((LEAF, PC), BF16),
        vmem((NY, NZ, R, R), F32), vmem((NZ, NY * R, R), BF16), vmem((NZ, NY * R, R), BF16),
        vmem((NZ, PC, R), F32), vmem((NY, PC, R), F32), vmem((PC, NY * R), BF16), vmem((PC, NY * R), BF16),
        vmem((NY, R, R), F32), vmem((NC, R, R), F32),
        vmem((NZ, PC, R), F32), vmem((2, QUARTERS, NZ // 2, QROWS, R), F32), vmem((NY, PC, R), F32),
        vmem((2, QUARTERS, NY // 2, QROWS, R), F32),
        vmem((R, R), F32), vmem((NZ, PIECE, R), F32), vmem((PIECE, R), F32), vmem((NC, PIECE, R), F32),
        vmem((NC, PIECE, R), F32), vmem((NC, PIECE, R), F32), vmem((PIECE, R), F32), vmem((R, R), F32), vmem((PC, R), F32),
        pltpu.SemaphoreType.DMA((N_LOCAL,)), pltpu.SemaphoreType.DMA((N_REMOTE,)), pltpu.SemaphoreType.DMA((N_REMOTE,)),
    ]
    near, total = pl.pallas_call(
        kernel,
        out_shape=(jax.ShapeDtypeStruct((LEAF, PC), F32), jax.ShapeDtypeStruct((PC, R), F32)),
        in_specs=[hbm] * 6,
        out_specs=[pl.BlockSpec(memory_space=pl.ANY)] * 2,
        scratch_shapes=scratch,
        compiler_params=pltpu.CompilerParams(collective_id=0, has_side_effects=True, vmem_limit_bytes=34 * 2**20),
    )(*[pltpu.with_memory_space_constraint(v, pltpu.HBM) for v in arrays])
    return pl.pallas_call(
        last,
        out_shape=jax.ShapeDtypeStruct((LEAF, PC), F32),
        in_specs=[pl.BlockSpec(memory_space=vmem)] * 3,
        out_specs=hbm,
        scratch_shapes=[vmem((LEAF, PC), F32), pltpu.SemaphoreType.DMA((4,))],
        compiler_params=pltpu.CompilerParams(vmem_limit_bytes=16 * 2**20),
    )(near, leaf_basis, total)


def solution(mesh):
    both = P(("cluster", "leaf"), None)
    return jax.shard_map(
        local,
        mesh=mesh,
        in_specs=(
            both, both, both, P(("cluster", "leaf"), None, None, None), P(("cluster", "leaf"), None, None),
            P("cluster", None, None, None),
        ),
        out_specs=both,
        check_vma=False,
    )
```

```python
import jax
import jax.numpy as jnp
from jax import lax
from jax.experimental import pallas as pl
from jax.experimental.pallas import tpu as pltpu
from jax.sharding import PartitionSpec as P

MESH = pl.DeviceIdType.MESH
F32, BF16 = jnp.float32, jnp.bfloat16
NY, NZ, NC = 4, 8, 8
LEAF, R, PC = 1024, 128, 512
HALF = PC // 2
NN = (((1,), (0,)), ((), ()))
NT = (((1,), (1,)), ((), ()))


def split(v):
    hi = v.astype(BF16)
    return hi, (v - hi.astype(F32)).astype(BF16)


def dot3(a, b, dims):
    (ah, al), (bh, bl) = a, b

    def one(u, v):
        return lax.dot_general(u, v, dims, preferred_element_type=F32)

    return one(ah, bh) + one(ah, bl) + one(al, bh)


GROUPS = ((4,), (3, 5), (2, 6), (1, 7))
QUARTERS, QROWS = 4, PC // 4
PIECE = R // NZ
ORDER = {1: (0, 1, 2, 3), -1: (2, 3, 0, 1)}


def steps(sign, quarter, size):
    return size // 2 if quarter in ORDER[sign][:2] else size // 2 - 1


def kernel(
    x_hbm, d_hbm, u_hbm, a_hbm, e_hbm, b_hbm, near_out, tot_out,
    near, tot, av, xv, dv, uv, xh, xl, a2, ah, al, cc, cr, crh, crl, er, bv, p2, rz, p1, ry, gs, gz, gp, gx, ts, tx, hp, hz,
    lsem, ssem, rsem,
):
    leaf = lax.axis_index("leaf")
    clu = lax.axis_index("cluster")
    y, z = leaf // NZ, lax.rem(leaf, NZ)
    ids = {}

    def number(kind, key):
        return ids.setdefault((kind, key), sum(k == kind for k, _ in ids))

    def at_y(d):
        return {"leaf": lax.rem(y + d + NY, NY) * NZ + z}

    def at_z(d):
        return {"leaf": y * NZ + lax.rem(z + d + NZ, NZ)}

    def at_c(d):
        return {"cluster": lax.rem(clu + d + NC, NC)}

    barrier = pltpu.get_barrier_semaphore()
    partners = [at_y(d) for d in range(1, NY)] + [at_z(d) for d in range(1, NZ)] + [at_c(d) for d in range(1, NC)]
    for partner in partners:
        pl.semaphore_signal(barrier, inc=1, device_id=partner, device_id_type=MESH)

    def load(src, dst, key):
        copy = pltpu.make_async_copy(src, dst, lsem.at[number("local", key)])
        copy.start()

    def send(src, dst, where, out, key):
        pltpu.make_async_remote_copy(
            src_ref=src, dst_ref=dst, send_sem=ssem.at[number("send", out)], recv_sem=rsem.at[number("recv", key)],
            device_id=where, device_id_type=MESH,
        ).start()

    def wait(kind, ref, key):
        sem = {"local": lsem, "send": ssem, "recv": rsem}[kind].at[ids[kind, key]]
        pltpu.make_async_copy(ref, ref, sem).wait()

    load(u_hbm, uv, "u")
    load(e_hbm.at[0], er.at[0], "e")
    XROWS = LEAF // 4
    for i in range(4):
        part = pl.ds(i * XROWS, XROWS)
        load(x_hbm.at[part], xv.at[part], ("x", i))

    wait("local", uv, "u")
    uh, ul = split(uv[...].T)
    coef = jnp.zeros((R, PC), F32)
    for i in range(4):
        part = slice(i * XROWS, (i + 1) * XROWS)
        wait("local", xv.at[pl.ds(i * XROWS, XROWS)], ("x", i))
        if i == 3:
            load(a_hbm.at[0], av, "a")
            load(d_hbm, dv, "d")
            for d in range(1, NY):
                load(a_hbm.at[0, lax.rem(y + d, NY) * NZ + z], a2.at[d, 0], "own_y")
            for d in range(1, NZ):
                load(a_hbm.at[0, y * NZ + lax.rem(z + d, NZ)], a2.at[0, d], "own_a")
            for d in range(1, NC):
                load(b_hbm.at[0, lax.rem(clu - d + NC, NC)], bv.at[d], "b")
        h, l = split(xv[part, :])
        xh[part, :] = h
        xl[part, :] = l
        coef = coef + dot3((uh[:, part], ul[:, part]), (h, l), NN)
    coef = coef.T
    cc[0] = coef
    cr[0] = coef

    pl.semaphore_wait(barrier, len(partners))

    def rows(quarter):
        return pl.ds(quarter * QROWS, QROWS)

    PAIR = pl.ds(0, 2 * QROWS)

    def gather_step(ref, size, where, sign, place, step):
        def slot(n):
            return (-sign * n) % size

        part = rows(ORDER[sign][place])
        send(ref.at[slot(step - 1), part], ref.at[slot(step), part], where(sign), ("gather", size), ("gather", size, place, step))

    def gather_event(ref, size, where, k):
        step, place = k // QUARTERS + 1, k % QUARTERS
        wait("recv", ref.at[0, PAIR], ("gather", size, place, step))
        for sign in (1, -1):
            if step < steps(sign, ORDER[sign][place], size):
                gather_step(ref, size, where, sign, place, step + 1)

    def z_event(k):
        gather_event(cc, NZ, at_z, k)

    def y_event(k):
        gather_event(cr, NY, at_y, k)

    for place in range(QUARTERS):
        for sign in (1, -1):
            gather_step(cc, NZ, at_z, sign, place, 1)
        for sign in (1, -1):
            gather_step(cr, NY, at_y, sign, place, 1)

    def send_cores(group):
        for d in group:
            for dy in (2, 1, 3):
                target = lax.rem(y + dy, NY) * NZ + lax.rem(z + d, NZ)
                send(av.at[target], a2.at[NY - dy, d], at_y(dy), "cores", ("cores", d))

    def near_chunk(i):
        size = LEAF // 4
        part = slice(i * size, (i + 1) * size)
        sym = dv[part, :] + dv[:, part].T
        near[part, :] = dot3(split(sym), (xh[...], xl[...]), NN)
        load(near.at[part], near_out.at[part], "near")

    wait("local", er.at[0], "e")
    for dy in (1, 3, 2):
        send(er.at[0], er.at[NY - dy], at_y(dy), "maps", "maps")
    z_event(0)
    y_event(0)
    z_event(1)
    y_event(1)
    wait("local", av, "a")
    send_cores(GROUPS[0])
    z_event(2)
    z_event(3)
    wait("local", dv, "d")
    near_chunk(0)
    z_event(4)
    y_event(2)
    y_event(3)
    send_cores(GROUPS[1])
    z_event(5)
    y_event(4)
    y_event(5)
    send_cores(GROUPS[2])
    send_cores(GROUPS[3])
    z_event(6)

    for r in range(NY):
        h, l = split(cr[r])
        crh[:, r * R : (r + 1) * R] = h
        crl[:, r * R : (r + 1) * R] = l
    z_event(7)

    wait("recv", er.at[pl.ds(1, NY - 1)], "maps")
    mine = pl.ds(pl.multiple_of(y * R, R), R)
    g = jnp.zeros((R, R), F32)
    for r in range(NY):
        g = g + dot3(split(cr[r, mine, :]), split(er[r]), NN)
    gs[...] = g

    def piece(at):
        return pl.ds(pl.multiple_of(at * PIECE, PIECE), PIECE)

    for d in (4, 3, 5, 2, 6, 1, 7):
        send(gs.at[piece(lax.rem(z + d, NZ))], gz.at[d], at_z(d), "gz", "gz")
    z_event(8)
    z_event(9)

    wait("local", a2.at[0, pl.ds(1, NZ - 1)], "own_a")

    def second(group):
        for d in group:
            wait("recv", a2.at[pl.ds(1, NY - 1), d], ("cores", d))
            h, l = split(a2[:, d].reshape(NY * R, R))
            ah[d] = h
            al[d] = l
        b = tuple(jnp.concatenate([m[d] for d in group], axis=1) for m in (ah, al))
        t = dot3((crh[...], crl[...]), b, NN)
        for i, d in enumerate(group):
            p2[d] = t[:, i * R : (i + 1) * R]

    def sum_step(ref, got, size, where, place, step):
        if step > 0:
            wait("recv", ref.at[0, PAIR], ("sum", size, place, step - 1))
        for way, sign in enumerate((1, -1)):
            quarter = ORDER[sign][place]
            at = (sign * (steps(sign, quarter, size) - step)) % size
            part = rows(quarter)
            if step > 0:
                ref[at, part] = ref[at, part] + got[way, quarter, step - 1]
            send(ref.at[at, part], got.at[way, quarter, step], where(sign), ("sum", size), ("sum", size, place, step))

    def sum_last(ref, got, size, place):
        for way, sign in enumerate((1, -1)):
            quarter = ORDER[sign][place]
            length = steps(sign, quarter, size)
            if way == 0:
                wait("recv", ref.at[0, PAIR], ("sum", size, place, length - 1))
            tot[rows(quarter), :] = tot[rows(quarter), :] + got[way, quarter, length - 1]

    def sum_steps(places, step):
        for place in places:
            sum_step(p2, rz, NZ, at_z, place, step)

    def first(group, fresh, part=range(NY)):
        a = split(jnp.concatenate([cc[d] for d in group], axis=1))
        b = tuple(jnp.concatenate([m[d, part[0] * R : (part[-1] + 1) * R] for d in group], axis=1) for m in (ah, al))
        t = dot3(a, b, NT)
        for i, r in enumerate(part):
            new = t[:, i * R : (i + 1) * R]
            p1[r] = new if fresh and r == 0 else p1[r] + new

    second(GROUPS[0])
    sum_steps((0, 1), 0)
    near_chunk(1)

    wait("local", a2.at[pl.ds(1, NY - 1), 0], "own_y")
    own = split(jnp.concatenate([a2[d, 0] for d in range(1, NY)], axis=1))
    t = dot3((crh[:, :R], crl[:, :R]), own, NN)
    for d in range(1, NY):
        p1[d] = t[:, (d - 1) * R : d * R]
    p2[0] = dot3((crh[:, R:], crl[:, R:]), own, NT)

    wait("recv", gz.at[pl.ds(1, NZ - 1)], "gz")
    own_piece = gs[piece(z), :]
    for d in range(1, NZ):
        own_piece = own_piece + gz[d]
    gp[...] = own_piece
    for d in range(1, NC):
        send(gp, gx.at[d], at_c(d), "gx", "gx")
    wait("local", bv.at[pl.ds(1, NC - 1)], "b")
    halves = split(own_piece)
    for d in range(1, NC):
        ts[d] = dot3(halves, split(bv[d]), NN)
    for d in range(1, NC):
        send(ts.at[d], tx.at[d], at_c(-d), "tx", "tx")

    second(GROUPS[1])
    sum_steps((2, 3), 0)
    for k in range(10, 14):
        z_event(k)
    first(GROUPS[0], True)
    sum_steps((0, 1), 1)

    wait("recv", gx.at[pl.ds(1, NC - 1)], "gx")
    wait("recv", tx.at[pl.ds(1, NC - 1)], "tx")
    field = tx[1]
    for d in range(2, NC):
        field = field + tx[d]
    for d in range(1, NC):
        field = field + dot3(split(gx[d]), split(bv[d]), NT)
    hp[...] = field
    hz[piece(z), :] = field
    for d in (4, 3, 5, 2, 6, 1, 7):
        send(hp, hz.at[piece(z)], at_z(d), "hz", "hz")

    first(GROUPS[1], False)
    second(GROUPS[2])
    sum_steps((2, 3), 1)
    near_chunk(2)
    sum_steps((0, 1), 2)
    first(GROUPS[2], False)

    wait("recv", hz.at[pl.ds(0, R - PIECE)], "hz")
    t = dot3(split(hz[...]), split(er[...].reshape(NY * R, R)), NT)
    for r in range(NY):
        p1[r, mine, :] = p1[r, mine, :] + t[:, r * R : (r + 1) * R]
    second(GROUPS[3])

    first(GROUPS[3], False, range(2, 4))
    for place in (0, 1):
        sum_step(p1, ry, NY, at_y, place, 0)
    first(GROUPS[3], False, range(0, 2))
    for place in (2, 3):
        sum_step(p1, ry, NY, at_y, place, 0)
    sum_steps((2, 3), 2)
    near_chunk(3)
    for place in (0, 1):
        sum_step(p2, rz, NZ, at_z, place, 3)
        sum_step(p1, ry, NY, at_y, place, 1)

    tot[...] = p1[0] + p2[0]
    for place in (2, 3, 0, 1):
        sum_last(p2, rz, NZ, place)
    for place in (2, 3, 0, 1):
        sum_last(p1, ry, NY, place)
    load(tot, tot_out, "tot")
    for size, ref in ((NZ, cc), (NY, cr)):
        for what in ("gather", "sum"):
            wait("send", ref.at[pl.ds(1, size - 1)], (what, size))
    wait("send", a2.at[pl.ds(1, NY - 1), pl.ds(1, NZ - 1)], "cores")
    wait("send", er.at[pl.ds(1, NY - 1)], "maps")
    wait("send", gz.at[pl.ds(1, NZ - 1)], "gz")
    wait("send", gx.at[pl.ds(1, NC - 1)], "gx")
    wait("send", tx.at[pl.ds(1, NC - 1)], "tx")
    wait("send", hz.at[pl.ds(0, R - PIECE)], "hz")
    wait("local", near, "near")
    wait("local", tot, "tot")


def last(near, u, tot, out, held, sems):
    high, low = split(tot[...])
    twice = jnp.concatenate([high, high], axis=1)
    copies = []
    for i in range(4):
        part = pl.ds(i * (LEAF // 4), LEAF // 4)
        h, l = split(u[part, :])
        far = lax.dot_general(jnp.concatenate([h, l], axis=1), twice, NT, preferred_element_type=F32)
        held[part, :] = near[part, :] + (far + lax.dot_general(h, low, NT, preferred_element_type=F32))
        copies.append(pltpu.make_async_copy(held.at[part], out.at[part], sems.at[i]))
        copies[-1].start()
    for copy in copies:
        copy.wait()


N_LOCAL, N_SEND, N_RECV = 13, 10, 52


def local(probes, dense_leaf, leaf_basis, sibling_cores, transfer, cluster_cores):
    arrays = (probes, dense_leaf, leaf_basis, sibling_cores, transfer, cluster_cores)
    hbm = pl.BlockSpec(memory_space=pltpu.HBM)
    vmem = pltpu.VMEM
    scratch = [
        vmem((LEAF, PC), F32), vmem((PC, R), F32), vmem((NY * NZ, R, R), F32), vmem((LEAF, PC), F32), vmem((LEAF, LEAF), F32), vmem((LEAF, R), F32), vmem((LEAF, PC), BF16), vmem((LEAF, PC), BF16),
        vmem((NY, NZ, R, R), F32), vmem((NZ, NY * R, R), BF16), vmem((NZ, NY * R, R), BF16),
        vmem((NZ, PC, R), F32), vmem((NY, PC, R), F32), vmem((PC, NY * R), BF16), vmem((PC, NY * R), BF16),
        vmem((NY, R, R), F32), vmem((NC, R, R), F32),
        vmem((NZ, PC, R), F32), vmem((2, QUARTERS, NZ // 2, QROWS, R), F32), vmem((NY, PC, R), F32),
        vmem((2, QUARTERS, NY // 2, QROWS, R), F32),
        vmem((R, R), F32), vmem((NZ, PIECE, R), F32), vmem((PIECE, R), F32), vmem((NC, PIECE, R), F32),
        vmem((NC, PIECE, R), F32), vmem((NC, PIECE, R), F32), vmem((PIECE, R), F32), vmem((R, R), F32),
        pltpu.SemaphoreType.DMA((N_LOCAL,)), pltpu.SemaphoreType.DMA((N_SEND,)), pltpu.SemaphoreType.DMA((N_RECV,)),
    ]
    near, total = pl.pallas_call(
        kernel,
        out_shape=(jax.ShapeDtypeStruct((LEAF, PC), F32), jax.ShapeDtypeStruct((PC, R), F32)),
        in_specs=[hbm] * 6,
        out_specs=[pl.BlockSpec(memory_space=pl.ANY)] * 2,
        scratch_shapes=scratch,
        compiler_params=pltpu.CompilerParams(collective_id=0, has_side_effects=True, vmem_limit_bytes=34 * 2**20),
    )(*[pltpu.with_memory_space_constraint(v, pltpu.HBM) for v in arrays])
    return pl.pallas_call(
        last,
        out_shape=jax.ShapeDtypeStruct((LEAF, PC), F32),
        in_specs=[pl.BlockSpec(memory_space=vmem)] * 3,
        out_specs=hbm,
        scratch_shapes=[vmem((LEAF, PC), F32), pltpu.SemaphoreType.DMA((4,))],
        compiler_params=pltpu.CompilerParams(vmem_limit_bytes=16 * 2**20),
    )(near, leaf_basis, total)


def solution(mesh):
    both = P(("cluster", "leaf"), None)
    return jax.shard_map(
        local,
        mesh=mesh,
        in_specs=(
            both, both, both, P(("cluster", "leaf"), None, None, None), P(("cluster", "leaf"), None, None),
            P("cluster", None, None, None),
        ),
        out_specs=both,
        check_vma=False,
    )
```

```python
import jax
import jax.numpy as jnp
from jax import lax
from jax.experimental import pallas as pl
from jax.experimental.pallas import tpu as pltpu
from jax.sharding import PartitionSpec as P

MESH = pl.DeviceIdType.MESH
F32, BF16 = jnp.float32, jnp.bfloat16
NY, NZ, NC = 4, 8, 8
LEAF, R, PC = 1024, 128, 512
HALF = PC // 2
NN = (((1,), (0,)), ((), ()))
NT = (((1,), (1,)), ((), ()))


def split(v):
    hi = v.astype(BF16)
    return hi, (v - hi.astype(F32)).astype(BF16)


def dot3(a, b, dims):
    (ah, al), (bh, bl) = a, b

    def one(u, v):
        return lax.dot_general(u, v, dims, preferred_element_type=F32)

    return one(ah, bh) + one(ah, bl) + one(al, bh)


GROUPS = ((4,), (3, 5), (2, 6), (1, 7))
QUARTERS, QROWS = 4, PC // 4
PIECE = R // NZ
ORDER = {1: (0, 1, 2, 3), -1: (2, 3, 0, 1)}


def steps(sign, quarter, size):
    return size // 2 if quarter in ORDER[sign][:2] else size // 2 - 1


def kernel(
    x_hbm, d_hbm, u_hbm, a_hbm, e_hbm, b_hbm, near_out, tot_out,
    near, tot, av, xv, dv, uv, xh, xl, a2, ah, al, cc, cr, crh, crl, er, bv, p2, rz, p1, ry, gs, gz, gp, gx, ts, tx, hp, hz,
    lsem, ssem, rsem,
):
    leaf = lax.axis_index("leaf")
    clu = lax.axis_index("cluster")
    y, z = leaf // NZ, lax.rem(leaf, NZ)
    ids = {}

    def number(kind, key):
        return ids.setdefault((kind, key), sum(k == kind for k, _ in ids))

    def at_y(d):
        return {"leaf": lax.rem(y + d + NY, NY) * NZ + z}

    def at_z(d):
        return {"leaf": y * NZ + lax.rem(z + d + NZ, NZ)}

    def at_c(d):
        return {"cluster": lax.rem(clu + d + NC, NC)}

    barrier = pltpu.get_barrier_semaphore()
    partners = [at_z(d) for d in (1, 7, 2, 6, 3, 5, 4)] + [at_y(d) for d in range(1, NY)] + [at_c(d) for d in range(1, NC)]
    for partner in partners:
        pl.semaphore_signal(barrier, inc=1, device_id=partner, device_id_type=MESH)

    def load(src, dst, key):
        copy = pltpu.make_async_copy(src, dst, lsem.at[number("local", key)])
        copy.start()

    def send(src, dst, where, out, key):
        pltpu.make_async_remote_copy(
            src_ref=src, dst_ref=dst, send_sem=ssem.at[number("send", out)], recv_sem=rsem.at[number("recv", key)],
            device_id=where, device_id_type=MESH,
        ).start()

    def wait(kind, ref, key):
        sem = {"local": lsem, "send": ssem, "recv": rsem}[kind].at[ids[kind, key]]
        pltpu.make_async_copy(ref, ref, sem).wait()

    load(u_hbm, uv, "u")
    load(e_hbm.at[0], er.at[0], "e")
    XROWS = LEAF // 4
    for i in range(4):
        part = pl.ds(i * XROWS, XROWS)
        load(x_hbm.at[part], xv.at[part], ("x", i))

    wait("local", uv, "u")
    uh, ul = split(uv[...].T)
    coef = jnp.zeros((R, PC), F32)
    for i in range(4):
        part = slice(i * XROWS, (i + 1) * XROWS)
        wait("local", xv.at[pl.ds(i * XROWS, XROWS)], ("x", i))
        if i == 3:
            load(a_hbm.at[0], av, "a")
            load(d_hbm, dv, "d")
            for d in range(1, NY):
                load(a_hbm.at[0, lax.rem(y + d, NY) * NZ + z], a2.at[d, 0], "own_y")
            for d in range(1, NZ):
                load(a_hbm.at[0, y * NZ + lax.rem(z + d, NZ)], a2.at[0, d], "own_a")
            for d in range(1, NC):
                load(b_hbm.at[0, lax.rem(clu - d + NC, NC)], bv.at[d], "b")
        h, l = split(xv[part, :])
        xh[part, :] = h
        xl[part, :] = l
        coef = coef + dot3((uh[:, part], ul[:, part]), (h, l), NN)
    coef = coef.T
    cc[0] = coef
    cr[0] = coef

    pl.semaphore_wait(barrier, len(partners))

    def rows(quarter):
        return pl.ds(quarter * QROWS, QROWS)

    PAIR = pl.ds(0, 2 * QROWS)

    def gather_step(ref, size, where, sign, place, step):
        def slot(n):
            return (-sign * n) % size

        part = rows(ORDER[sign][place])
        send(ref.at[slot(step - 1), part], ref.at[slot(step), part], where(sign), ("gather", size), ("gather", size, place, step))

    def gather_event(ref, size, where, k):
        step, place = k // QUARTERS + 1, k % QUARTERS
        wait("recv", ref.at[0, PAIR], ("gather", size, place, step))
        for sign in (1, -1):
            if step < steps(sign, ORDER[sign][place], size):
                gather_step(ref, size, where, sign, place, step + 1)

    def z_event(k):
        gather_event(cc, NZ, at_z, k)

    def y_event(k):
        gather_event(cr, NY, at_y, k)

    for place in range(QUARTERS):
        for sign in (1, -1):
            gather_step(cc, NZ, at_z, sign, place, 1)
        for sign in (1, -1):
            gather_step(cr, NY, at_y, sign, place, 1)

    def send_cores(group):
        for d in group:
            for dy in (2, 1, 3):
                target = lax.rem(y + dy, NY) * NZ + lax.rem(z + d, NZ)
                send(av.at[target], a2.at[NY - dy, d], at_y(dy), "cores", ("cores", d))

    def near_chunk(i):
        size = LEAF // 4
        part = slice(i * size, (i + 1) * size)
        sym = dv[part, :] + dv[:, part].T
        near[part, :] = dot3(split(sym), (xh[...], xl[...]), NN)
        load(near.at[part], near_out.at[part], "near")

    wait("local", er.at[0], "e")
    for dy in (1, 3, 2):
        send(er.at[0], er.at[NY - dy], at_y(dy), "maps", "maps")
    z_event(0)
    y_event(0)
    z_event(1)
    y_event(1)
    wait("local", av, "a")
    send_cores(GROUPS[0])
    z_event(2)
    z_event(3)
    wait("local", dv, "d")
    near_chunk(0)
    z_event(4)
    y_event(2)
    y_event(3)
    send_cores(GROUPS[1])
    z_event(5)
    y_event(4)
    y_event(5)
    send_cores(GROUPS[2])
    send_cores(GROUPS[3])
    z_event(6)

    for r in range(NY):
        h, l = split(cr[r])
        crh[:, r * R : (r + 1) * R] = h
        crl[:, r * R : (r + 1) * R] = l
    z_event(7)

    wait("recv", er.at[pl.ds(1, NY - 1)], "maps")
    mine = pl.ds(pl.multiple_of(y * R, R), R)
    g = jnp.zeros((R, R), F32)
    for r in range(NY):
        g = g + dot3(split(cr[r, mine, :]), split(er[r]), NN)
    gs[...] = g

    def piece(at):
        return pl.ds(pl.multiple_of(at * PIECE, PIECE), PIECE)

    for d in (4, 3, 5, 2, 6, 1, 7):
        send(gs.at[piece(lax.rem(z + d, NZ))], gz.at[d], at_z(d), "gz", "gz")
    z_event(8)
    z_event(9)

    wait("local", a2.at[0, pl.ds(1, NZ - 1)], "own_a")

    def second(group):
        for d in group:
            wait("recv", a2.at[pl.ds(1, NY - 1), d], ("cores", d))
            h, l = split(a2[:, d].reshape(NY * R, R))
            ah[d] = h
            al[d] = l
        b = tuple(jnp.concatenate([m[d] for d in group], axis=1) for m in (ah, al))
        t = dot3((crh[...], crl[...]), b, NN)
        for i, d in enumerate(group):
            p2[d] = t[:, i * R : (i + 1) * R]

    def sum_step(ref, got, size, where, place, step):
        if step > 0:
            wait("recv", ref.at[0, PAIR], ("sum", size, place, step - 1))
        for way, sign in enumerate((1, -1)):
            quarter = ORDER[sign][place]
            at = (sign * (steps(sign, quarter, size) - step)) % size
            part = rows(quarter)
            if step > 0:
                ref[at, part] = ref[at, part] + got[way, quarter, step - 1]
            send(ref.at[at, part], got.at[way, quarter, step], where(sign), ("sum", size), ("sum", size, place, step))

    def sum_last(ref, got, size, place):
        for way, sign in enumerate((1, -1)):
            quarter = ORDER[sign][place]
            length = steps(sign, quarter, size)
            if way == 0:
                wait("recv", ref.at[0, PAIR], ("sum", size, place, length - 1))
            tot[rows(quarter), :] = tot[rows(quarter), :] + got[way, quarter, length - 1]

    def sum_steps(places, step):
        for place in places:
            sum_step(p2, rz, NZ, at_z, place, step)

    def first(group, fresh, part=range(NY)):
        a = split(jnp.concatenate([cc[d] for d in group], axis=1))
        b = tuple(jnp.concatenate([m[d, part[0] * R : (part[-1] + 1) * R] for d in group], axis=1) for m in (ah, al))
        t = dot3(a, b, NT)
        for i, r in enumerate(part):
            new = t[:, i * R : (i + 1) * R]
            p1[r] = new if fresh and r == 0 else p1[r] + new

    second(GROUPS[0])
    sum_steps((0, 1), 0)
    near_chunk(1)

    wait("local", a2.at[pl.ds(1, NY - 1), 0], "own_y")
    own = split(jnp.concatenate([a2[d, 0] for d in range(1, NY)], axis=1))
    t = dot3((crh[:, :R], crl[:, :R]), own, NN)
    for d in range(1, NY):
        p1[d] = t[:, (d - 1) * R : d * R]
    p2[0] = dot3((crh[:, R:], crl[:, R:]), own, NT)

    wait("recv", gz.at[pl.ds(1, NZ - 1)], "gz")
    own_piece = gs[piece(z), :]
    for d in range(1, NZ):
        own_piece = own_piece + gz[d]
    gp[...] = own_piece
    for d in range(1, NC):
        send(gp, gx.at[d], at_c(d), "gx", "gx")
    wait("local", bv.at[pl.ds(1, NC - 1)], "b")
    halves = split(own_piece)
    for d in range(1, NC):
        ts[d] = dot3(halves, split(bv[d]), NN)
    for d in range(1, NC):
        send(ts.at[d], tx.at[d], at_c(-d), "tx", "tx")

    second(GROUPS[1])
    sum_steps((2, 3), 0)
    for k in range(10, 14):
        z_event(k)
    first(GROUPS[0], True)
    sum_steps((0, 1), 1)

    wait("recv", gx.at[pl.ds(1, NC - 1)], "gx")
    wait("recv", tx.at[pl.ds(1, NC - 1)], "tx")
    field = tx[1]
    for d in range(2, NC):
        field = field + tx[d]
    for d in range(1, NC):
        field = field + dot3(split(gx[d]), split(bv[d]), NT)
    hp[...] = field
    hz[piece(z), :] = field
    for d in (4, 3, 5, 2, 6, 1, 7):
        send(hp, hz.at[piece(z)], at_z(d), "hz", "hz")

    first(GROUPS[1], False)
    second(GROUPS[2])
    sum_steps((2, 3), 1)
    near_chunk(2)
    sum_steps((0, 1), 2)
    first(GROUPS[2], False)

    wait("recv", hz.at[pl.ds(0, R - PIECE)], "hz")
    t = dot3(split(hz[...]), split(er[...].reshape(NY * R, R)), NT)
    for r in range(NY):
        p1[r, mine, :] = p1[r, mine, :] + t[:, r * R : (r + 1) * R]
    second(GROUPS[3])

    first(GROUPS[3], False, range(2, 4))
    for place in (0, 1):
        sum_step(p1, ry, NY, at_y, place, 0)
    first(GROUPS[3], False, range(0, 2))
    for place in (2, 3):
        sum_step(p1, ry, NY, at_y, place, 0)
    sum_steps((2, 3), 2)
    near_chunk(3)
    for place in (0, 1):
        sum_step(p2, rz, NZ, at_z, place, 3)
        sum_step(p1, ry, NY, at_y, place, 1)

    tot[...] = p1[0] + p2[0]
    for place in (2, 3, 0, 1):
        sum_last(p2, rz, NZ, place)
    for place in (2, 3, 0, 1):
        sum_last(p1, ry, NY, place)
    load(tot, tot_out, "tot")
    for size, ref in ((NZ, cc), (NY, cr)):
        for what in ("gather", "sum"):
            wait("send", ref.at[pl.ds(1, size - 1)], (what, size))
    wait("send", a2.at[pl.ds(1, NY - 1), pl.ds(1, NZ - 1)], "cores")
    wait("send", er.at[pl.ds(1, NY - 1)], "maps")
    wait("send", gz.at[pl.ds(1, NZ - 1)], "gz")
    wait("send", gx.at[pl.ds(1, NC - 1)], "gx")
    wait("send", tx.at[pl.ds(1, NC - 1)], "tx")
    wait("send", hz.at[pl.ds(0, R - PIECE)], "hz")
    wait("local", near, "near")
    wait("local", tot, "tot")


def last(near, u, tot, out, held, sems):
    high, low = split(tot[...])
    twice = jnp.concatenate([high, high], axis=1)
    copies = []
    for i in range(4):
        part = pl.ds(i * (LEAF // 4), LEAF // 4)
        h, l = split(u[part, :])
        far = lax.dot_general(jnp.concatenate([h, l], axis=1), twice, NT, preferred_element_type=F32)
        held[part, :] = near[part, :] + (far + lax.dot_general(h, low, NT, preferred_element_type=F32))
        copies.append(pltpu.make_async_copy(held.at[part], out.at[part], sems.at[i]))
        copies[-1].start()
    for copy in copies:
        copy.wait()


N_LOCAL, N_SEND, N_RECV = 13, 10, 52


def local(probes, dense_leaf, leaf_basis, sibling_cores, transfer, cluster_cores):
    arrays = (probes, dense_leaf, leaf_basis, sibling_cores, transfer, cluster_cores)
    hbm = pl.BlockSpec(memory_space=pltpu.HBM)
    vmem = pltpu.VMEM
    scratch = [
        vmem((LEAF, PC), F32), vmem((PC, R), F32), vmem((NY * NZ, R, R), F32), vmem((LEAF, PC), F32), vmem((LEAF, LEAF), F32), vmem((LEAF, R), F32), vmem((LEAF, PC), BF16), vmem((LEAF, PC), BF16),
        vmem((NY, NZ, R, R), F32), vmem((NZ, NY * R, R), BF16), vmem((NZ, NY * R, R), BF16),
        vmem((NZ, PC, R), F32), vmem((NY, PC, R), F32), vmem((PC, NY * R), BF16), vmem((PC, NY * R), BF16),
        vmem((NY, R, R), F32), vmem((NC, R, R), F32),
        vmem((NZ, PC, R), F32), vmem((2, QUARTERS, NZ // 2, QROWS, R), F32), vmem((NY, PC, R), F32),
        vmem((2, QUARTERS, NY // 2, QROWS, R), F32),
        vmem((R, R), F32), vmem((NZ, PIECE, R), F32), vmem((PIECE, R), F32), vmem((NC, PIECE, R), F32),
        vmem((NC, PIECE, R), F32), vmem((NC, PIECE, R), F32), vmem((PIECE, R), F32), vmem((R, R), F32),
        pltpu.SemaphoreType.DMA((N_LOCAL,)), pltpu.SemaphoreType.DMA((N_SEND,)), pltpu.SemaphoreType.DMA((N_RECV,)),
    ]
    near, total = pl.pallas_call(
        kernel,
        out_shape=(jax.ShapeDtypeStruct((LEAF, PC), F32), jax.ShapeDtypeStruct((PC, R), F32)),
        in_specs=[hbm] * 6,
        out_specs=[pl.BlockSpec(memory_space=pl.ANY)] * 2,
        scratch_shapes=scratch,
        compiler_params=pltpu.CompilerParams(collective_id=0, has_side_effects=True, vmem_limit_bytes=34 * 2**20),
    )(*[pltpu.with_memory_space_constraint(v, pltpu.HBM) for v in arrays])
    return pl.pallas_call(
        last,
        out_shape=jax.ShapeDtypeStruct((LEAF, PC), F32),
        in_specs=[pl.BlockSpec(memory_space=vmem)] * 3,
        out_specs=hbm,
        scratch_shapes=[vmem((LEAF, PC), F32), pltpu.SemaphoreType.DMA((4,))],
        compiler_params=pltpu.CompilerParams(vmem_limit_bytes=16 * 2**20),
    )(near, leaf_basis, total)


def solution(mesh):
    both = P(("cluster", "leaf"), None)
    return jax.shard_map(
        local,
        mesh=mesh,
        in_specs=(
            both, both, both, P(("cluster", "leaf"), None, None, None), P(("cluster", "leaf"), None, None),
            P("cluster", None, None, None),
        ),
        out_specs=both,
        check_vma=False,
    )
```
